32 devices in a mesh: groups: 2 (over x), att: 2 (over y), exp: 8 (over z, core).
Axes of the slice: x: 2, y: 2, z: 4, core: 2. Of those that a mesh axis runs over, the one named last changes fastest.
Arguments:
- queries: bfloat16 [1024, 4096], P(('groups', 'exp')), parts along dimension 0, may hold values from -12 to 12
- row_key_value: bfloat16 [1024, 1024], P(('groups', 'exp')), parts along dimension 0, may hold values from -12 to 12
- shared_context_cache: bfloat16 [4, 1024, 1024], P('groups', 'att'), parts along dimension 0, may hold values from -6 to 6
- branch: int32 [1024], P(('groups', 'exp')), parts along dimension 0, may hold values from 0 to 1
- sink_logits: float32 [64], replicated, may hold values from 8 to 13
- w_out: bfloat16 [4096, 2880], P(None, 'att'), may hold values from -0.09375 to 0.09375
- residual: bfloat16 [1024, 2880], P(('groups', 'exp'), 'att'), parts along dimension 0, may hold values from -20 to 20
- norm_gain: bfloat16 [2880], P('att'), may hold values from 0.099609375 to 1.8984375
- expert_ids: int32 [1024, 4], P(('groups', 'exp')), parts along dimension 0, may hold values from 0 to 7, all different within a row; in each aligned block of 64 rows (0 to 63, 64 to 127, ...) at most 64 rows name the same one
- weight_codes: int32 [1024, 4], P(('groups', 'exp')), parts along dimension 0, may hold values from 1 to 255
- w_gate: bfloat16 [8, 2880, 2880], P('exp', None, 'att'), may hold values from -0.4375 to 0.4375
- w_up: bfloat16 [8, 2880, 2880], P('exp', None, 'att'), may hold values from -0.4375 to 0.4375
- w_down: bfloat16 [8, 2880, 2880], P('exp', 'att'), may hold values from -0.013671875 to 0.013671875
Outputs:
- attended: bfloat16 [1024, 2880], P(('groups', 'exp'), 'att'), parts along dimension 0
- expert_mix: bfloat16 [1024, 2880], P(('groups', 'exp'), 'att'), parts along dimension 0
The draws below stay inside these ranges and needn't reach their ends.
There are 2 independent parts, one for each index of `groups`. The reference program is written for one: setup_inputs(seed, part) draws one part's arguments, and reference() takes and returns one part's arrays. A program takes and returns all parts, laid end to end along the dimension named above; an argument that names none is the same for every part. Nothing has to cross between parts.
Inputs may be any that keep to these rules, and one draw needn't show every extreme that they name: `expert_ids`: each row names 4 different experts; within the rows of one index of exp (aligned blocks of 64 rows) no expert is named more than 64 times, and in some block some expert is named exactly 64 times.
All inputs are finite; a program needn't handle non-finite values.
Results may differ from the reference program's by a relative error of at most 0.022.
Values may be sent and summed in bfloat16 or wider, within the bound.
No kernel may reach another device: no remote copies, remote signals or barrier semaphores. Data moves between devices by JAX's collectives and lax.ppermute only.
A program may use at most 128 MiB of HBM per device.

```python
import math
from functools import partial
import jax
import jax.numpy as jnp
import numpy as np
from jax import lax

D = 2880
QUERY_HEADS = 64
KEY_VALUE_HEADS = 8
HEAD_SIZE = 64
FF = 2880
TOP = 4
SHARED_CONTEXTS = 2
ROWS_DEV = 64
EXPERTS = 8
DECODE_ROWS = 512
CONTEXT_TOKENS = 1024
CAP = 64
N_EXP = 8


def draw_queries(key, part):
    random_seed_key = jax.random.fold_in(key, 11)
    value_rows = jnp.clip(2.5 * jax.random.normal(random_seed_key, (DECODE_ROWS, QUERY_HEADS, HEAD_SIZE), jnp.float32), -12.0, 12.0)
    return value_rows.reshape(DECODE_ROWS, QUERY_HEADS * HEAD_SIZE).astype(jnp.bfloat16)


def draw_shared_context_cache(key, part):
    random_seed_key = jax.random.fold_in(key, 12)
    value_rows = jnp.clip(jax.random.normal(random_seed_key, (SHARED_CONTEXTS, CONTEXT_TOKENS, 2, KEY_VALUE_HEADS, HEAD_SIZE), jnp.float32), -6.0, 6.0)
    return value_rows.reshape(SHARED_CONTEXTS, CONTEXT_TOKENS, 2 * KEY_VALUE_HEADS * HEAD_SIZE).astype(jnp.bfloat16)


def draw_residual(key, part):
    column = jnp.arange(D, dtype=jnp.float32) / (D - 1)
    random_seed_key = jax.random.fold_in(key, 13)
    value_rows = jnp.clip(jax.random.normal(random_seed_key, (DECODE_ROWS, D), jnp.float32), -6.0, 6.0) * 0.4 * jnp.exp(column * math.log(3.0))[None, :]
    return value_rows.astype(jnp.bfloat16)


def plant(result, own_key, least, largest):
    shape = result.shape
    place = [jax.random.randint(jax.random.fold_in(own_key, axis), (), 0, shape[axis]) for axis in range(len(shape))]
    result = result.at[tuple(place)].set(least)
    longest = shape.index(max(shape))
    place[longest] = (place[longest] + 1) % shape[longest]
    return result.at[tuple(place)].set(largest)


def steps_of(key, extent, cuts, low, high):
    factor_of, own = 1.0, jax.random.fold_in(key, 6)
    for axis_at, parts in cuts:
        steps = jnp.exp(jax.random.uniform(jax.random.fold_in(own, axis_at), (parts,), jnp.float32, low / len(cuts), high / len(cuts)))
        factor_of = factor_of * jnp.repeat(steps, extent[axis_at] // parts).reshape([-1 if axis == axis_at else 1 for axis in range(len(extent))])
    return factor_of


def deal_out(own_key, own, number, rows, amount, top, most, skew):
    order = jax.random.permutation(own_key, amount)
    crowded, usual = load_shares(amount, rows * top, most, skew, True), load_shares(amount, rows * top, most, skew, False)
    places = jnp.arange(amount)

    def named(sizes, turn):
        used = int((sizes > 0).sum())
        fixed = max(1, used // 4)
        passed = fixed + (places - fixed + turn * (used - fixed)) % max(1, amount - fixed)
        return jnp.zeros((amount,), jnp.int32).at[order[jnp.where(places < fixed, places, passed)]].set(jnp.asarray(sizes, jnp.int32))

    sizes = jnp.where(number % 4 == 0, named(crowded, number // 4), named(usual, number - number // 4 - 1))
    mixed = jax.random.permutation(jax.random.fold_in(own, 3), amount)
    donor, taker = mixed[0:amount // 2 * 2:2], mixed[1:amount // 2 * 2:2]
    slack = jnp.minimum(sizes[donor] - 1, most - sizes[taker]) // 2
    slack = jnp.where((donor == order[0]) | (taker == order[0]) | (sizes[taker] == 0), 0, jnp.maximum(slack, 0))
    passed = jax.random.randint(jax.random.fold_in(own, 4), (amount // 2,), 0, 1 << 20) % (slack + 1)
    sizes = sizes.at[donor].add(-passed).at[taker].add(passed)
    labels = jnp.searchsorted(jnp.cumsum(sizes), jnp.arange(rows * top), side="right").astype(jnp.int32)
    listing = labels.reshape(top, rows).T
    listing = listing[jax.random.permutation(jax.random.fold_in(own, 1), rows)]
    turn = jax.random.randint(jax.random.fold_in(own, 2), (rows, 1), 0, top)
    return jnp.take_along_axis(listing, (jnp.arange(top)[None, :] + turn) % top, axis=1)


def load_shares(amount, total, most, skew, full):
    portions = [(1 << 20) // math.isqrt(grade ** skew) + 1 for grade in range(1, amount + 1)]
    largest = most if full else min(most, max(-(-total // amount), total * portions[0] // sum(portions)))
    least = 1 if total - largest >= amount - 1 else 0
    given, rest = [largest] + [least] * (amount - 1), total - largest - least * (amount - 1)
    while rest > 0:
        free = [i for i in range(1, amount) if given[i] < largest] or [i for i in range(1, amount) if given[i] < most]
        mass, left = sum([portions[i] for i in free]), rest
        for i in free:
            extra = min(most - given[i], max(1, left * portions[i] // mass), rest)
            given[i] = given[i] + extra
            rest = rest - extra
    return np.array(given)


def centred(rng, extent, width, bound, cuts=(), kind=jnp.bfloat16):
    loudness = steps_of(rng, extent, cuts, -0.22, 0.18) if cuts else 1.0
    result = jax.random.normal(rng, extent, jnp.float32) * width * loudness
    return jnp.minimum(jnp.maximum(result, -bound), bound).astype(kind)


def setup_inputs(seed: int = 0, part: int = 0) -> dict:
    keys = jax.random.split(jax.random.key(seed), 14)
    part_splits = jax.random.split(jax.random.fold_in(keys[13], part), 14)
    queries = draw_queries(jax.random.fold_in(jax.random.fold_in(keys[13], part), 71), part)
    row_key_value = centred(part_splits[1], (DECODE_ROWS, 2 * KEY_VALUE_HEADS * HEAD_SIZE), 2.0, 12.0, ((0, 8),))
    shared_context_cache = draw_shared_context_cache(jax.random.fold_in(jax.random.fold_in(keys[13], part), 71), part)
    branch = plant(jax.random.randint(part_splits[3], (DECODE_ROWS,), 0, SHARED_CONTEXTS), jax.random.fold_in(part_splits[3], 1), 0, SHARED_CONTEXTS - 1).astype(jnp.int32)
    sink_logits = jnp.clip(jax.random.uniform(keys[4], (QUERY_HEADS,), jnp.float32, 8.0, 13.0), 8.0, 13.0)
    w_out = centred(keys[5], (QUERY_HEADS * HEAD_SIZE, D), (QUERY_HEADS * HEAD_SIZE) ** -0.5, 0.09375, ((1, 2),))
    residual = draw_residual(jax.random.fold_in(jax.random.fold_in(keys[13], part), 71), part)
    norm_gain = jnp.clip(1.0 + 0.18 * jax.random.normal(keys[7], (D,), jnp.float32), 0.099609375, 1.8984375).astype(jnp.bfloat16)
    expert_ids_keys = jax.random.split(jax.random.fold_in(part_splits[8], 1), DECODE_ROWS // ROWS_DEV)
    expert_ids_turns = jax.random.permutation(jax.random.fold_in(part_splits[8], 3), DECODE_ROWS // ROWS_DEV)
    expert_ids = jax.vmap(lambda own, number: deal_out(jax.random.fold_in(part_splits[8], 2), own, number, ROWS_DEV, EXPERTS, TOP, CAP, 2))(expert_ids_keys, expert_ids_turns).reshape((DECODE_ROWS, TOP))
    weight_codes = plant(jax.random.randint(part_splits[9], (DECODE_ROWS, TOP), 1, 256), jax.random.fold_in(part_splits[9], 1), 1, 255).astype(jnp.int32)
    w_gate = centred(keys[10], (EXPERTS, D, FF), (D // 16) ** -0.5, 0.4375, ((0, 8), (2, 2)))
    w_up = centred(keys[11], (EXPERTS, D, FF), (D // 16) ** -0.5, 0.4375, ((0, 8), (2, 2)))
    w_down = centred(keys[12], (EXPERTS, FF, D), (64 * FF) ** -0.5, 0.013671875, ((0, 8), (1, 2)))
    return {"queries": queries, "row_key_value": row_key_value, "shared_context_cache": shared_context_cache, "branch": branch, "sink_logits": sink_logits, "w_out": w_out, "residual": residual, "norm_gain": norm_gain, "expert_ids": expert_ids, "weight_codes": weight_codes, "w_gate": w_gate, "w_up": w_up, "w_down": w_down}


clamp_limit = 7.0

def attend_block(packed, shared_context_cache, sink_logits):
    query_block, fresh_block, block_branch = packed
    decode_row_count = query_block.shape[0]
    heads_per_group = QUERY_HEADS // KEY_VALUE_HEADS
    score_scale = HEAD_SIZE ** (-0.5)
    grouped_heads = query_block.reshape(decode_row_count, KEY_VALUE_HEADS, heads_per_group, HEAD_SIZE).astype(jnp.float32)
    current = None
    for context_slot in range(SHARED_CONTEXTS):
        cached_key_block = shared_context_cache[context_slot, :, :KEY_VALUE_HEADS * HEAD_SIZE].reshape(-1, KEY_VALUE_HEADS, HEAD_SIZE).astype(jnp.float32)
        cached_value_block = shared_context_cache[context_slot, :, KEY_VALUE_HEADS * HEAD_SIZE:].reshape(-1, KEY_VALUE_HEADS, HEAD_SIZE).astype(jnp.float32)
        scores = jnp.einsum('rgqd,tgd->rgqt', grouped_heads, cached_key_block) * score_scale
        local_max = lax.optimization_barrier(jnp.max(scores, axis=-1))
        weights = jnp.exp(scores - local_max[..., None])
        local_total = lax.optimization_barrier(jnp.sum(weights, axis=-1))
        rounded = lax.optimization_barrier(weights.astype(jnp.bfloat16)).astype(jnp.float32)
        local_out = jnp.einsum('rgqt,tgd->rgqd', rounded, cached_value_block)
        if current is None:
            current = (local_max, local_total, local_out)
        else:
            chosen = block_branch == context_slot
            current = (jnp.where(chosen[:, None, None], local_max, current[0]), jnp.where(chosen[:, None, None], local_total, current[1]), jnp.where(chosen[:, None, None, None], local_out, current[2]))
    cache_max = current[0].reshape(decode_row_count, QUERY_HEADS)
    cache_total = current[1].reshape(decode_row_count, QUERY_HEADS)
    cache_out = current[2].reshape(decode_row_count, QUERY_HEADS, HEAD_SIZE)
    row_own_keys = fresh_block[:, :KEY_VALUE_HEADS * HEAD_SIZE].reshape(decode_row_count, KEY_VALUE_HEADS, 1, HEAD_SIZE).astype(jnp.float32)
    row_own_values = fresh_block[:, KEY_VALUE_HEADS * HEAD_SIZE:].reshape(decode_row_count, KEY_VALUE_HEADS, 1, HEAD_SIZE).astype(jnp.float32)
    own_score = (lax.optimization_barrier(jnp.sum(grouped_heads * row_own_keys, axis=-1)) * score_scale).reshape(decode_row_count, QUERY_HEADS)
    row_own_values = jnp.broadcast_to(row_own_values, (decode_row_count, KEY_VALUE_HEADS, heads_per_group, HEAD_SIZE)).reshape(decode_row_count, QUERY_HEADS, HEAD_SIZE)
    sink_row = sink_logits.astype(jnp.float32)[None, :]
    peak = jnp.maximum(jnp.maximum(cache_max, own_score), sink_row)
    cache_factor = jnp.exp(cache_max - peak)
    own_factor = jnp.exp(own_score - peak)
    sink_factor = jnp.exp(sink_row - peak)
    denominator = cache_total * cache_factor + own_factor + sink_factor
    numerator = cache_out * cache_factor[..., None] + own_factor[..., None] * row_own_values
    return (numerator / denominator[..., None]).reshape(decode_row_count, QUERY_HEADS * HEAD_SIZE).astype(jnp.bfloat16)

def reference(queries, row_key_value, shared_context_cache, branch, sink_logits, w_out, residual, norm_gain, expert_ids, weight_codes, w_gate, w_up, w_down):
    total_rows = queries.shape[0]
    blocks = total_rows // ROWS_DEV
    packed = (queries.reshape(blocks, ROWS_DEV, -1), row_key_value.reshape(blocks, ROWS_DEV, -1), branch.reshape(blocks, ROWS_DEV))
    attention = lax.map(partial(attend_block, shared_context_cache=shared_context_cache, sink_logits=sink_logits), packed)
    attention = attention.reshape(total_rows, QUERY_HEADS * HEAD_SIZE)
    hidden = residual.astype(jnp.float32) + jnp.dot(attention, w_out, preferred_element_type=jnp.float32)
    attended = hidden.astype(jnp.bfloat16)
    squares = lax.optimization_barrier(jnp.sum(hidden * hidden, axis=1))
    inverse = lax.rsqrt(squares / D + 1e-05)
    normed = (hidden * inverse[:, None] * norm_gain.astype(jnp.float32)[None, :]).astype(jnp.bfloat16)
    shares = weight_codes.astype(jnp.float32)
    shares = shares / lax.optimization_barrier(jnp.sum(shares, axis=1, keepdims=True))
    room = N_EXP * CAP

    def one_expert(mixture, packed_expert):
        expert, gate_weight, up_weight, down_weight = packed_expert
        expert_hit = expert_ids == expert
        routed = jnp.any(expert_hit, axis=1)
        share = lax.optimization_barrier(jnp.sum(jnp.where(expert_hit, shares, jnp.zeros_like(shares)), axis=1))
        chosen = jnp.nonzero(routed, size=room, fill_value=0)[0].astype(jnp.int32)
        valid = (jnp.arange(room, dtype=jnp.int32) < jnp.sum(routed.astype(jnp.int32))).astype(jnp.float32)
        rows_in = normed[chosen]
        gate_sum = jnp.minimum(jnp.dot(rows_in, gate_weight, preferred_element_type=jnp.float32), clamp_limit)
        up_sum = jnp.clip(jnp.dot(rows_in, up_weight, preferred_element_type=jnp.float32), -clamp_limit, clamp_limit)
        active = (gate_sum * jax.nn.sigmoid(1.702 * gate_sum) * (up_sum + 1.0)).astype(jnp.bfloat16)
        output = jnp.dot(active, down_weight, preferred_element_type=jnp.float32).astype(jnp.bfloat16)
        contribution = output.astype(jnp.float32) * (share[chosen] * valid)[:, None]
        return (mixture.at[chosen].add(contribution), None)
    start_mix = jnp.zeros((total_rows, D), jnp.float32)
    mixture, ignored = lax.scan(one_expert, start_mix, (jnp.arange(EXPERTS, dtype=jnp.int32), w_gate, w_up, w_down))
    return (attended, mixture.astype(jnp.bfloat16))
```

```python
import functools

import jax
import jax.numpy as jnp
from jax import lax
from jax.experimental import pallas as pl
from jax.experimental.pallas import tpu as pltpu
from jax.sharding import PartitionSpec as P

D = 2880
QUERY_HEADS = 64
KEY_VALUE_HEADS = 8
HEAD_SIZE = 64
TOP = 4
SHARED_CONTEXTS = 2
LANES = 128
GROUP = QUERY_HEADS // KEY_VALUE_HEADS
CHUNKS = 2
CHUNK_HEADS = QUERY_HEADS // CHUNKS
CHUNK_COLUMNS = CHUNK_HEADS * HEAD_SIZE
PAIR_COLUMNS = 2 * GROUP * HEAD_SIZE
STEPS = CHUNK_COLUMNS // PAIR_COLUMNS
FAR = -1e30

clamp_limit = 7.0


VMEM_SPEC = pl.BlockSpec(memory_space=pltpu.VMEM)
SMEM_SPEC = pl.BlockSpec(memory_space=pltpu.SMEM)
ANY_SPEC = pl.BlockSpec(memory_space=pl.ANY)


def split(x):
    high = x.astype(jnp.bfloat16)
    return high, (x - high.astype(jnp.float32)).astype(jnp.bfloat16)


def nt_dot(a, b):
    return lax.dot_general(a, b, (((1,), (1,)), ((), ())), preferred_element_type=jnp.float32)


def dot(a, b):
    return jnp.dot(a, b, preferred_element_type=jnp.float32)


def attend_kernel(chunk, place, sinks, branch, queries, keys, values, own_keys, own_values, out):
    step = pl.program_id(0)
    rows = queries.shape[0]
    first = place[0] == 0
    lane = lax.broadcasted_iota(jnp.int32, (rows, LANES), 1)
    low = lane < HEAD_SIZE
    second_context = jnp.broadcast_to(branch[...], (rows, LANES)) == 1
    second_all = jnp.concatenate([second_context] * GROUP, axis=0)
    key_pair = jnp.concatenate([keys[0], keys[1]], axis=1)
    value_pair = jnp.concatenate([values[0], values[1]], axis=1)
    own_key = own_keys[...].astype(jnp.float32)
    own_value = own_values[...].astype(jnp.float32)
    stats = jnp.zeros((rows, LANES), jnp.float32)
    for j in range(2):
        wanted = low if j == 0 else jnp.logical_not(low)
        pieces = []
        for pair in range(GROUP // 2):
            start = (j * GROUP + 2 * pair) * HEAD_SIZE
            both = queries[:, start : start + LANES].astype(jnp.float32) * HEAD_SIZE**-0.5
            turned = pltpu.roll(both, HEAD_SIZE, 1)
            even, odd = (both, turned) if j == 0 else (turned, both)
            pieces.append(jnp.where(wanted, even, 0.0))
            pieces.append(jnp.where(wanted, odd, 0.0))
        grouped = jnp.concatenate(pieces, axis=0)
        spread = jnp.concatenate(
            [jnp.where(second_all, 0.0, grouped), jnp.where(second_all, grouped, 0.0)], axis=1
        ).astype(jnp.bfloat16)
        scores = nt_dot(spread, key_pair)
        own = jnp.sum(grouped * jnp.concatenate([own_key] * GROUP, axis=0), axis=1, keepdims=True)
        head0 = chunk * CHUNK_HEADS + step * 2 * GROUP + j * GROUP
        sink = jnp.concatenate(
            [jnp.full((rows, 1), sinks[head0 + h], jnp.float32) for h in range(GROUP)], axis=0
        )
        own = jnp.where(first, own, FAR)
        sink = jnp.where(first, sink, FAR)
        peak = jnp.maximum(jnp.max(scores, axis=1, keepdims=True), jnp.maximum(own, sink))
        peak = peak.astype(jnp.bfloat16).astype(jnp.float32)
        weights = jnp.exp(scores - peak)
        own_weight = jnp.exp(own - peak)
        total = jnp.sum(weights, axis=1, keepdims=True) + own_weight + jnp.exp(sink - peak)
        mixed = dot(weights.astype(jnp.bfloat16), value_pair)
        mixed = jnp.where(second_all, mixed[:, LANES:], mixed[:, :LANES])
        mixed = mixed + own_weight * jnp.concatenate([own_value] * GROUP, axis=0)
        high = total.astype(jnp.bfloat16).astype(jnp.float32)
        rest = total - high
        for h in range(GROUP):
            at = step * 2 * GROUP + j * GROUP + h
            here = slice(h * rows, (h + 1) * rows)
            stats = jnp.where(lane == at, peak[here], stats)
            stats = jnp.where(lane == at + CHUNK_HEADS, high[here], stats)
            stats = jnp.where(lane == at + 2 * CHUNK_HEADS, rest[here], stats)
        for pair in range(GROUP // 2):
            even = mixed[2 * pair * rows : (2 * pair + 1) * rows]
            odd = mixed[(2 * pair + 1) * rows : (2 * pair + 2) * rows]
            if j == 0:
                odd = pltpu.roll(odd, HEAD_SIZE, 1)
            else:
                even = pltpu.roll(even, HEAD_SIZE, 1)
            start = pl.multiple_of(
                step * PAIR_COLUMNS + (j * GROUP + 2 * pair) * HEAD_SIZE, LANES
            )
            out[:, pl.ds(start, LANES)] = jnp.where(low, even, odd).astype(jnp.bfloat16)
    mine = jnp.logical_or(
        jnp.logical_or(lane // (2 * GROUP) == step, lane // (2 * GROUP) == step + STEPS),
        lane // (2 * GROUP) == step + 2 * STEPS,
    )
    tail = slice(CHUNK_COLUMNS, CHUNK_COLUMNS + LANES)

    @pl.when(step == 0)
    def _():
        out[:, tail] = jnp.zeros((rows, LANES), jnp.bfloat16)

    before = out[:, tail].astype(jnp.float32)
    out[:, tail] = jnp.where(mine, stats, before).astype(jnp.bfloat16)


def attend(chunk, place, sinks, branch, queries, cache, row_key_value):
    rows = queries.shape[0]
    tokens = cache.shape[1]
    half = KEY_VALUE_HEADS * HEAD_SIZE // LANES
    at = lambda s: chunk * STEPS + s
    return pl.pallas_call(
        functools.partial(attend_kernel, chunk),
        grid=(STEPS,),
        in_specs=[
            SMEM_SPEC,
            SMEM_SPEC,
            pl.BlockSpec((rows, 1), lambda s: (0, 0)),
            pl.BlockSpec((rows, PAIR_COLUMNS), lambda s: (0, at(s))),
            pl.BlockSpec((SHARED_CONTEXTS, tokens, LANES), lambda s: (0, 0, at(s))),
            pl.BlockSpec((SHARED_CONTEXTS, tokens, LANES), lambda s: (0, 0, half + at(s))),
            pl.BlockSpec((rows, LANES), lambda s: (0, at(s))),
            pl.BlockSpec((rows, LANES), lambda s: (0, half + at(s))),
        ],
        out_specs=pl.BlockSpec((rows, CHUNK_COLUMNS + LANES), lambda s: (0, 0)),
        out_shape=jax.ShapeDtypeStruct((rows, CHUNK_COLUMNS + LANES), jnp.bfloat16),
        compiler_params=pltpu.CompilerParams(vmem_limit_bytes=16 << 20),
        cost_estimate=pl.CostEstimate(
            flops=4 * rows * CHUNK_HEADS * tokens * LANES * 2,
            transcendentals=rows * CHUNK_HEADS * tokens,
            bytes_accessed=2 << 20,
        ),
        name=f"attend{chunk}",
    )(place, sinks, branch, queries, cache, cache, row_key_value, row_key_value)


def merged_product(parts, w_out, base):
    rows = parts[0].shape[0]
    tops, totals = [], []
    for part in parts:
        stats = part[:, CHUNK_COLUMNS : CHUNK_COLUMNS + LANES].astype(jnp.float32)
        tops.append(stats[:, :CHUNK_HEADS])
        totals.append(
            stats[:, CHUNK_HEADS : 2 * CHUNK_HEADS] + stats[:, 2 * CHUNK_HEADS : 3 * CHUNK_HEADS]
        )
    top = functools.reduce(jnp.maximum, tops)
    factors = [jnp.exp(t - top) for t in tops]
    whole = functools.reduce(jnp.add, [f * t for f, t in zip(factors, totals)])
    factor = jnp.concatenate([f / whole for f in factors], axis=0)
    high, rest = split(factor)
    factor = jnp.concatenate([high, rest], axis=1)
    width = GROUP * HEAD_SIZE
    total = None
    for j in range(CHUNK_COLUMNS // width):
        head = lax.broadcasted_iota(jnp.int32, (2 * CHUNK_HEADS, width), 0) % CHUNK_HEADS
        column = lax.broadcasted_iota(jnp.int32, (2 * CHUNK_HEADS, width), 1)
        spread = (head == j * GROUP + column // HEAD_SIZE).astype(jnp.bfloat16)
        scale = dot(factor, spread)
        mixed = None
        for i, part in enumerate(parts):
            term = part[:, j * width : (j + 1) * width].astype(jnp.float32)
            term = term * scale[i * rows : (i + 1) * rows]
            mixed = term if mixed is None else mixed + term
        term = nt_dot(mixed.astype(jnp.bfloat16), w_out[:, base + j * width : base + (j + 1) * width])
        total = term if total is None else total + term
    return total


def project_kernel(n, chunk, *refs):
    parts, (w_out, out) = refs[:n], refs[n:]
    out[...] = merged_product(parts, w_out, chunk * CHUNK_COLUMNS)


def finish_kernel(n, chunk, experts, *refs):
    parts = refs[:n]
    w_out, so_far, residual, gain, ids, codes, attended, packed = refs[n:]
    rows, width = residual.shape
    hidden = (
        residual[...].astype(jnp.float32) + so_far[...] + merged_product(parts, w_out, chunk * CHUNK_COLUMNS)
    )
    attended[...] = hidden.astype(jnp.bfloat16)
    packed[:, :width] = (hidden * gain[...].astype(jnp.float32)).astype(jnp.bfloat16)
    spare = packed.shape[1] - width
    lane = lax.broadcasted_iota(jnp.int32, (rows, spare), 1)
    squares = jnp.sum(hidden * hidden, axis=1, keepdims=True)
    code = codes[...].astype(jnp.float32)
    whole = code[:, 0:1]
    for k in range(1, TOP):
        whole = whole + code[:, k : k + 1]
    extra = jnp.zeros((rows, spare), jnp.float32)
    high = squares.astype(jnp.bfloat16).astype(jnp.float32)
    extra = jnp.where(lane == 0, high, extra)
    extra = jnp.where(lane == 1, squares - high, extra)
    for k in range(TOP):
        share = code[:, k : k + 1] / whole
        high = share.astype(jnp.bfloat16).astype(jnp.float32)
        expert = ids[:, k : k + 1]
        extra = jnp.where(lane == 2 + expert, high, extra)
        extra = jnp.where(lane == 2 + experts + expert, share - high, extra)
    packed[:, width:] = extra.astype(jnp.bfloat16)


def packed_width(width, experts):
    return -(-(width + 2 + 2 * experts) // LANES) * LANES


def project(parts, w_out, chunk):
    rows = parts[0].shape[0]
    width = w_out.shape[0]
    n = len(parts)
    whole = lambda shape: pl.BlockSpec(shape, lambda i: (0,) * len(shape))
    return pl.pallas_call(
        functools.partial(project_kernel, n, chunk),
        grid=(1,),
        in_specs=[whole(parts[0].shape)] * n
        + [VMEM_SPEC],
        out_specs=whole((rows, width)),
        out_shape=jax.ShapeDtypeStruct((rows, width), jnp.float32),
        compiler_params=pltpu.CompilerParams(vmem_limit_bytes=16 << 20),
        cost_estimate=pl.CostEstimate(
            flops=2 * rows * CHUNK_COLUMNS * width * 4,
            transcendentals=0,
            bytes_accessed=2 * CHUNK_COLUMNS * width,
        ),
        name=f"project{chunk}",
    )(*parts, w_out)


def finish(parts, w_out, chunk, so_far, residual, gain, ids, codes, experts):
    rows, width = residual.shape
    n = len(parts)
    whole = lambda shape: pl.BlockSpec(shape, lambda i: (0,) * len(shape))
    wide = packed_width(width, experts)
    return pl.pallas_call(
        functools.partial(finish_kernel, n, chunk, experts),
        grid=(1,),
        in_specs=[whole(parts[0].shape)] * n
        + [
            VMEM_SPEC,
            whole((rows, width)),
            whole((rows, width)),
            whole((1, width)),
            whole((rows, TOP)),
            whole((rows, TOP)),
        ],
        out_specs=(whole((rows, width)), whole((rows, wide))),
        out_shape=(
            jax.ShapeDtypeStruct((rows, width), jnp.bfloat16),
            jax.ShapeDtypeStruct((rows, wide), jnp.bfloat16),
        ),
        compiler_params=pltpu.CompilerParams(vmem_limit_bytes=16 << 20),
        cost_estimate=pl.CostEstimate(
            flops=2 * rows * CHUNK_COLUMNS * width * 4,
            transcendentals=0,
            bytes_accessed=2 * CHUNK_COLUMNS * width,
        ),
        name="finish",
    )(*parts, w_out, so_far, residual, gain, ids, codes)


def expert_kernel(n, cores, experts, place, *refs):
    count = n * cores
    blocks = refs[:count]
    w_gate, w_up, w_down, kept, sent = refs[count:]
    rows = blocks[0].shape[0]
    width = w_gate.shape[1]
    own_part, expert = place[0], place[1]
    whole = [
        jnp.concatenate([blocks[c * n + k][...] for c in range(cores)], axis=0) for k in range(n)
    ]
    pieces = []
    for i in range(n):
        piece = whole[0][:, :width]
        for k in range(1, n):
            piece = jnp.where((own_part ^ k) == i, whole[k][:, :width], piece)
        pieces.append(piece)
    source = jnp.concatenate(pieces, axis=1)
    squares = None
    for k in range(n):
        extra = whole[k][:, width:].astype(jnp.float32)
        term = extra[:, 0:1] + extra[:, 1:2]
        squares = term if squares is None else squares + term
    extra = whole[0][:, width:].astype(jnp.float32)
    lane = lax.broadcasted_iota(jnp.int32, extra.shape, 1)
    hit = jnp.logical_or(lane == 2 + expert, lane == 2 + experts + expert)
    share = jnp.sum(jnp.where(hit, extra, 0.0), axis=1, keepdims=True)
    inverse = lax.rsqrt(squares / D + 1e-05)
    gate_sum = jnp.minimum(nt_dot(source, w_gate[0]) * inverse, clamp_limit)
    up_sum = jnp.clip(nt_dot(source, w_up[0]) * inverse, -clamp_limit, clamp_limit)
    active = gate_sum * jax.nn.sigmoid(1.702 * gate_sum) * (up_sum + 1.0)
    result = dot(active.astype(jnp.bfloat16), w_down[0]) * share
    halves = [result[:, i * width : (i + 1) * width] for i in range(n)]
    for k in range(n):
        piece = halves[0]
        for i in range(1, n):
            piece = jnp.where((own_part ^ k) == i, halves[i], piece)
        piece = piece.astype(jnp.bfloat16)
        kept[k] = piece[:rows]
        if cores > 1:
            sent[k] = piece[rows:]


def run_experts(blocks, n, cores, place, w_gate, w_up, w_down, experts, name):
    rows = blocks[0].shape[0]
    width = w_gate.shape[1]
    shape = jax.ShapeDtypeStruct((n, rows, width), jnp.bfloat16)
    return pl.pallas_call(
        functools.partial(expert_kernel, n, cores, experts),
        in_specs=[SMEM_SPEC] + [VMEM_SPEC] * (len(blocks) + 3),
        out_specs=(VMEM_SPEC, VMEM_SPEC),
        out_shape=(shape, shape),
        compiler_params=pltpu.CompilerParams(vmem_limit_bytes=20 << 20),
        cost_estimate=pl.CostEstimate(
            flops=6 * rows * cores * D * width * 2,
            transcendentals=rows * cores * width,
            bytes_accessed=6 * D * width,
        ),
        name=name,
    )(place, *blocks, w_gate, w_up, w_down)


def held(x):
    return pltpu.with_memory_space_constraint(x, pltpu.VMEM)


def shards(
    queries,
    row_key_value,
    shared_context_cache,
    branch,
    sink_logits,
    w_out,
    residual,
    norm_gain,
    expert_ids,
    weight_codes,
    w_gate,
    w_up,
    w_down,
):
    n = lax.axis_size("att")
    senders = lax.axis_size("exp")
    experts = w_gate.shape[0] * senders
    assert w_gate.shape[0] == 1 and n & (n - 1) == 0 and senders & (senders - 1) == 0
    cores = 2
    chips = senders // cores
    part = lax.axis_index("att")
    place = jnp.stack([part, lax.axis_index("exp")]).astype(jnp.int32)

    def over_att(x, k):
        return lax.ppermute(x, "att", [(i, i ^ k) for i in range(n)])

    def over_exp(x, k):
        return lax.ppermute(x, "exp", [(i, i ^ k) for i in range(senders)])

    w_out = held(w_out.T)
    w_gate = held(jnp.swapaxes(w_gate, 1, 2))
    w_up = held(jnp.swapaxes(w_up, 1, 2))
    w_down = held(w_down)
    gathered = []
    for chunk in range(CHUNKS):
        mine = attend(
            chunk, place, sink_logits, branch[:, None], queries, shared_context_cache, row_key_value
        )
        gathered.append([mine] + [over_att(mine, k) for k in range(1, n)])
    so_far = project(gathered[0], w_out, 0)
    attended, packed = finish(
        gathered[1],
        w_out,
        1,
        so_far,
        residual,
        norm_gain[None, :],
        expert_ids,
        weight_codes,
        experts,
    )
    home = None
    for chip in range(chips):
        block = packed if chip == 0 else over_exp(packed, chip * cores)
        parts = [block] + [over_att(block, k) for k in range(1, n)]
        blocks = parts + [over_exp(b, 1) for b in parts]
        kept, sent = run_experts(
            blocks, n, cores, place, w_gate, w_up, w_down, experts, f"experts{chip}"
        )
        other = over_exp(sent, 1)
        summed = kept.astype(jnp.float32) + other.astype(jnp.float32)
        own = summed[0]
        for k in range(1, n):
            own = own + over_att(summed[k].astype(jnp.bfloat16), k).astype(jnp.float32)
        if chip == 0:
            home = own
        else:
            back = over_exp(own.astype(jnp.bfloat16), chip * cores)
            home = home + back.astype(jnp.float32)
    return (attended, home.astype(jnp.bfloat16))


def solution(mesh):
    placed = (
        P(("groups", "exp"), None),
        P(("groups", "exp"), None),
        P("groups", "att", None),
        P(("groups", "exp")),
        P(),
        P(None, "att"),
        P(("groups", "exp"), "att"),
        P("att"),
        P(("groups", "exp"), None),
        P(("groups", "exp"), None),
        P("exp", None, "att"),
        P("exp", None, "att"),
        P("exp", "att", None),
    )
    return jax.shard_map(
        shards,
        mesh=mesh,
        in_specs=placed,
        out_specs=(P(("groups", "exp"), "att"), P(("groups", "exp"), "att")),
        check_vma=False,
    )
```

```python
import functools

import jax
import jax.numpy as jnp
from jax import lax
from jax.experimental import pallas as pl
from jax.experimental.pallas import tpu as pltpu
from jax.sharding import PartitionSpec as P


D = 2880
QUERY_HEADS = 64
KEY_VALUE_HEADS = 8
HEAD_SIZE = 64
TOP = 4
SHARED_CONTEXTS = 2
LANES = 128
GROUP = QUERY_HEADS // KEY_VALUE_HEADS
CHUNKS = 2
CHUNK_HEADS = QUERY_HEADS // CHUNKS
CHUNK_COLUMNS = CHUNK_HEADS * HEAD_SIZE
PAIR_COLUMNS = 2 * GROUP * HEAD_SIZE
STEPS = CHUNK_COLUMNS // PAIR_COLUMNS
FAR = -1e30

clamp_limit = 7.0


VMEM_SPEC = pl.BlockSpec(memory_space=pltpu.VMEM)
SMEM_SPEC = pl.BlockSpec(memory_space=pltpu.SMEM)
ANY_SPEC = pl.BlockSpec(memory_space=pl.ANY)


def split(x):
    high = x.astype(jnp.bfloat16)
    return high, (x - high.astype(jnp.float32)).astype(jnp.bfloat16)


def nt_dot(a, b):
    return lax.dot_general(a, b, (((1,), (1,)), ((), ())), preferred_element_type=jnp.float32)


def dot(a, b):
    return jnp.dot(a, b, preferred_element_type=jnp.float32)


def as_column(row, rows):
    across = lax.broadcasted_iota(jnp.int32, (rows, rows), 1)
    down = lax.broadcasted_iota(jnp.int32, (rows, rows), 0)
    square = jnp.broadcast_to(row, (rows, rows))
    return jnp.sum(jnp.where(across == down, square, jnp.zeros_like(square)), axis=1, keepdims=True)


def attend_kernel(
    chunk, place, sinks, branch, queries, keys, values, own_keys, own_values, w_out, out, w_held, sem
):
    step = pl.program_id(0)
    rows = queries.shape[0]
    fetch = pltpu.make_async_copy(
        w_out.at[:, chunk * CHUNK_COLUMNS : (chunk + 1) * CHUNK_COLUMNS], w_held, sem
    )

    @pl.when(step == 0)
    def _():
        fetch.start()

    first = place[0] == 0
    lane = lax.broadcasted_iota(jnp.int32, (rows, LANES), 1)
    low = lane < HEAD_SIZE
    branch_column = as_column(branch[...].astype(jnp.float32), rows)
    second_context = jnp.broadcast_to(branch_column, (rows, LANES)) == 1.0
    second_all = jnp.concatenate([second_context] * GROUP, axis=0)
    key_pair = jnp.concatenate([keys[0], keys[1]], axis=1)
    value_pair = jnp.concatenate([values[0], values[1]], axis=1)
    own_key = own_keys[...].astype(jnp.float32)
    own_value = own_values[...].astype(jnp.float32)
    stats = jnp.zeros((rows, LANES), jnp.float32)
    for j in range(2):
        wanted = low if j == 0 else jnp.logical_not(low)
        pieces = []
        for pair in range(GROUP // 2):
            start = (j * GROUP + 2 * pair) * HEAD_SIZE
            both = queries[:, start : start + LANES].astype(jnp.float32) * HEAD_SIZE**-0.5
            turned = pltpu.roll(both, HEAD_SIZE, 1)
            even, odd = (both, turned) if j == 0 else (turned, both)
            pieces.append(jnp.where(wanted, even, 0.0))
            pieces.append(jnp.where(wanted, odd, 0.0))
        grouped = jnp.concatenate(pieces, axis=0)
        spread = jnp.concatenate(
            [jnp.where(second_all, 0.0, grouped), jnp.where(second_all, grouped, 0.0)], axis=1
        ).astype(jnp.bfloat16)
        scores = nt_dot(spread, key_pair)
        own = jnp.sum(grouped * jnp.concatenate([own_key] * GROUP, axis=0), axis=1, keepdims=True)
        head0 = chunk * CHUNK_HEADS + step * 2 * GROUP + j * GROUP
        sink = jnp.concatenate(
            [jnp.full((rows, 1), sinks[head0 + h], jnp.float32) for h in range(GROUP)], axis=0
        )
        own = jnp.where(first, own, FAR)
        sink = jnp.where(first, sink, FAR)
        peak = jnp.maximum(jnp.max(scores, axis=1, keepdims=True), jnp.maximum(own, sink))
        peak = peak.astype(jnp.bfloat16).astype(jnp.float32)
        weights = jnp.exp(scores - peak)
        own_weight = jnp.exp(own - peak)
        total = jnp.sum(weights, axis=1, keepdims=True) + own_weight + jnp.exp(sink - peak)
        mixed = dot(weights.astype(jnp.bfloat16), value_pair)
        mixed = jnp.where(second_all, mixed[:, LANES:], mixed[:, :LANES])
        mixed = mixed + own_weight * jnp.concatenate([own_value] * GROUP, axis=0)
        high = total.astype(jnp.bfloat16).astype(jnp.float32)
        rest = total - high
        for h in range(GROUP):
            at = step * 2 * GROUP + j * GROUP + h
            here = slice(h * rows, (h + 1) * rows)
            stats = jnp.where(lane == at, peak[here], stats)
            stats = jnp.where(lane == at + CHUNK_HEADS, high[here], stats)
            stats = jnp.where(lane == at + 2 * CHUNK_HEADS, rest[here], stats)
        for pair in range(GROUP // 2):
            even = mixed[2 * pair * rows : (2 * pair + 1) * rows]
            odd = mixed[(2 * pair + 1) * rows : (2 * pair + 2) * rows]
            if j == 0:
                odd = pltpu.roll(odd, HEAD_SIZE, 1)
            else:
                even = pltpu.roll(even, HEAD_SIZE, 1)
            start = pl.multiple_of(
                step * PAIR_COLUMNS + (j * GROUP + 2 * pair) * HEAD_SIZE, LANES
            )
            out[:, pl.ds(start, LANES)] = jnp.where(low, even, odd).astype(jnp.bfloat16)
    mine = jnp.logical_or(
        jnp.logical_or(lane // (2 * GROUP) == step, lane // (2 * GROUP) == step + STEPS),
        lane // (2 * GROUP) == step + 2 * STEPS,
    )
    tail = slice(CHUNK_COLUMNS, CHUNK_COLUMNS + LANES)

    @pl.when(step == 0)
    def _():
        out[:, tail] = jnp.zeros((rows, LANES), jnp.bfloat16)

    before = out[:, tail].astype(jnp.float32)
    out[:, tail] = jnp.where(mine, stats, before).astype(jnp.bfloat16)

    @pl.when(step == STEPS - 1)
    def _():
        fetch.wait()


def attend(chunk, place, sinks, branch, queries, cache, row_key_value, w_out):
    rows = queries.shape[0]
    tokens = cache.shape[1]
    half = KEY_VALUE_HEADS * HEAD_SIZE // LANES
    at = lambda s: chunk * STEPS + s
    return pl.pallas_call(
        functools.partial(attend_kernel, chunk),
        grid=(STEPS,),
        in_specs=[
            SMEM_SPEC,
            SMEM_SPEC,
            pl.BlockSpec((1, rows), lambda s: (0, 0)),
            pl.BlockSpec((rows, PAIR_COLUMNS), lambda s: (0, at(s))),
            pl.BlockSpec((SHARED_CONTEXTS, tokens, LANES), lambda s: (0, 0, at(s))),
            pl.BlockSpec((SHARED_CONTEXTS, tokens, LANES), lambda s: (0, 0, half + at(s))),
            pl.BlockSpec((rows, LANES), lambda s: (0, at(s))),
            pl.BlockSpec((rows, LANES), lambda s: (0, half + at(s))),
            ANY_SPEC,
        ],
        out_specs=(
            pl.BlockSpec((rows, CHUNK_COLUMNS + LANES), lambda s: (0, 0)),
            ANY_SPEC,
        ),
        out_shape=(
            jax.ShapeDtypeStruct((rows, CHUNK_COLUMNS + LANES), jnp.bfloat16),
            pltpu.VMEM((w_out.shape[0], CHUNK_COLUMNS), jnp.bfloat16),
        ),
        scratch_shapes=[pltpu.SemaphoreType.DMA],
        compiler_params=pltpu.CompilerParams(vmem_limit_bytes=16 << 20),
        cost_estimate=pl.CostEstimate(
            flops=4 * rows * CHUNK_HEADS * tokens * LANES * 2,
            transcendentals=rows * CHUNK_HEADS * tokens,
            bytes_accessed=2 << 20,
        ),
    )(place, sinks, branch, queries, cache, cache, row_key_value, row_key_value, w_out)


def merged_product(parts, w_out, base):
    rows = parts[0].shape[0]
    tops, totals = [], []
    for part in parts:
        stats = part[:, CHUNK_COLUMNS : CHUNK_COLUMNS + LANES].astype(jnp.float32)
        tops.append(stats[:, :CHUNK_HEADS])
        totals.append(
            stats[:, CHUNK_HEADS : 2 * CHUNK_HEADS] + stats[:, 2 * CHUNK_HEADS : 3 * CHUNK_HEADS]
        )
    top = functools.reduce(jnp.maximum, tops)
    factors = [jnp.exp(t - top) for t in tops]
    whole = functools.reduce(jnp.add, [f * t for f, t in zip(factors, totals)])
    factor = jnp.concatenate([f / whole for f in factors], axis=0)
    high, rest = split(factor)
    factor = jnp.concatenate([high, rest], axis=1)
    width = GROUP * HEAD_SIZE
    total = None
    for j in range(CHUNK_COLUMNS // width):
        head = lax.broadcasted_iota(jnp.int32, (2 * CHUNK_HEADS, width), 0) % CHUNK_HEADS
        column = lax.broadcasted_iota(jnp.int32, (2 * CHUNK_HEADS, width), 1)
        spread = (head == j * GROUP + column // HEAD_SIZE).astype(jnp.bfloat16)
        scale = dot(factor, spread)
        mixed = None
        for i, part in enumerate(parts):
            term = part[:, j * width : (j + 1) * width].astype(jnp.float32)
            term = term * scale[i * rows : (i + 1) * rows]
            mixed = term if mixed is None else mixed + term
        term = nt_dot(mixed.astype(jnp.bfloat16), w_out[:, base + j * width : base + (j + 1) * width])
        total = term if total is None else total + term
    return total


def project_kernel(n, *refs):
    parts, (w_out, out) = refs[:n], refs[n:]
    out[...] = merged_product(parts, w_out, 0)


def finish_kernel(n, experts, *refs):
    parts = refs[:n]
    w_out, so_far, residual, gain, ids, codes, attended, packed = refs[n:]
    rows, width = residual.shape
    hidden = (
        residual[...].astype(jnp.float32) + so_far[...] + merged_product(parts, w_out, 0)
    )
    attended[...] = hidden.astype(jnp.bfloat16)
    packed[:, :width] = (hidden * gain[...].astype(jnp.float32)).astype(jnp.bfloat16)
    spare = packed.shape[1] - width
    lane = lax.broadcasted_iota(jnp.int32, (rows, spare), 1)
    squares = jnp.sum(hidden * hidden, axis=1, keepdims=True)
    code = codes[...].astype(jnp.float32)
    code = [as_column(code[k : k + 1], rows) for k in range(TOP)]
    whole = functools.reduce(jnp.add, code)
    experts_of = ids[...].astype(jnp.float32)
    experts_of = [as_column(experts_of[k : k + 1], rows).astype(jnp.int32) for k in range(TOP)]
    extra = jnp.zeros((rows, spare), jnp.float32)
    high = squares.astype(jnp.bfloat16).astype(jnp.float32)
    extra = jnp.where(lane == 0, high, extra)
    extra = jnp.where(lane == 1, squares - high, extra)
    for k in range(TOP):
        share = code[k] / whole
        high = share.astype(jnp.bfloat16).astype(jnp.float32)
        expert = experts_of[k]
        extra = jnp.where(lane == 2 + expert, high, extra)
        extra = jnp.where(lane == 2 + experts + expert, share - high, extra)
    packed[:, width:] = extra.astype(jnp.bfloat16)


def packed_width(width, experts):
    return -(-(width + 2 + 2 * experts) // LANES) * LANES


def project(parts, w_out):
    rows = parts[0].shape[0]
    width = w_out.shape[0]
    n = len(parts)
    whole = lambda shape: pl.BlockSpec(shape, lambda i: (0,) * len(shape))
    return pl.pallas_call(
        functools.partial(project_kernel, n),
        grid=(1,),
        in_specs=[whole(parts[0].shape)] * n
        + [VMEM_SPEC],
        out_specs=whole((rows, width)),
        out_shape=jax.ShapeDtypeStruct((rows, width), jnp.float32),
        compiler_params=pltpu.CompilerParams(vmem_limit_bytes=16 << 20),
        cost_estimate=pl.CostEstimate(
            flops=2 * rows * CHUNK_COLUMNS * width * 4,
            transcendentals=0,
            bytes_accessed=2 * CHUNK_COLUMNS * width,
        ),
    )(*parts, w_out)


def finish(parts, w_out, so_far, residual, gain, ids, codes, experts):
    rows, width = residual.shape
    n = len(parts)
    whole = lambda shape: pl.BlockSpec(shape, lambda i: (0,) * len(shape))
    wide = packed_width(width, experts)
    return pl.pallas_call(
        functools.partial(finish_kernel, n, experts),
        grid=(1,),
        in_specs=[whole(parts[0].shape)] * n
        + [
            VMEM_SPEC,
            whole((rows, width)),
            whole((rows, width)),
            whole((1, width)),
            whole((TOP, rows)),
            whole((TOP, rows)),
        ],
        out_specs=(whole((rows, width)), whole((rows, wide))),
        out_shape=(
            jax.ShapeDtypeStruct((rows, width), jnp.bfloat16),
            jax.ShapeDtypeStruct((rows, wide), jnp.bfloat16),
        ),
        compiler_params=pltpu.CompilerParams(vmem_limit_bytes=16 << 20),
        cost_estimate=pl.CostEstimate(
            flops=2 * rows * CHUNK_COLUMNS * width * 4,
            transcendentals=0,
            bytes_accessed=2 * CHUNK_COLUMNS * width,
        ),
        name="finish",
    )(*parts, w_out, so_far, residual, gain, ids, codes)


def stacked(blocks, n, cores, k):
    return jnp.concatenate([blocks[c * n + k][...] for c in range(cores)], axis=0)


def gate_kernel(n, cores, place, *refs):
    count = n * cores
    blocks = refs[:count]
    w_gate, w_up, active = refs[count:]
    width = w_gate.shape[1]
    own_part = place[0]
    whole = [stacked(blocks, n, cores, k) for k in range(n)]
    pieces = []
    for i in range(n):
        piece = whole[0][:, :width]
        for k in range(1, n):
            piece = jnp.where((own_part ^ k) == i, whole[k][:, :width], piece)
        pieces.append(piece)
    source = jnp.concatenate(pieces, axis=1)
    spare = blocks[0].shape[1] - width
    lane = lax.broadcasted_iota(jnp.int32, (8, spare), 1)
    first_two = (lane < 2).astype(jnp.bfloat16)
    squares = functools.reduce(jnp.add, [nt_dot(first_two, w[:, width:]) for w in whole])[0:1]
    inverse = lax.rsqrt(squares / D + 1e-05)
    gate_sum = jnp.minimum(nt_dot(w_gate[0], source) * inverse, clamp_limit)
    up_sum = jnp.clip(nt_dot(w_up[0], source) * inverse, -clamp_limit, clamp_limit)
    result = gate_sum * jax.nn.sigmoid(1.702 * gate_sum) * (up_sum + 1.0)
    active[...] = result.astype(jnp.bfloat16)


def down_kernel(n, cores, experts, place, *refs):
    blocks = refs[:cores]
    active, w_down = refs[cores : cores + 2]
    outs = refs[cores + 2 :]
    rows = blocks[0].shape[0]
    width = w_down.shape[1]
    own_part, expert = place[0], place[1]
    extra = stacked(blocks, 1, cores, 0)[:, width:].astype(jnp.float32)
    lane = lax.broadcasted_iota(jnp.int32, extra.shape, 1)
    hit = jnp.logical_or(lane == 2 + expert, lane == 2 + experts + expert)
    share = jnp.sum(jnp.where(hit, extra, 0.0), axis=1, keepdims=True)
    result = lax.dot_general(
        active[...], w_down[0], (((0,), (0,)), ((), ())), preferred_element_type=jnp.float32
    )
    result = result * share
    halves = [result[:, i * width : (i + 1) * width] for i in range(n)]
    for k in range(n):
        piece = halves[0]
        for i in range(1, n):
            piece = jnp.where((own_part ^ k) == i, halves[i], piece)
        piece = piece.astype(jnp.bfloat16)
        for i, out in enumerate(outs):
            out[k] = piece[i * rows : (i + 1) * rows]


def run_gate(blocks, n, cores, place, w_gate, w_up):
    rows = blocks[0].shape[0]
    width = w_gate.shape[1]
    return pl.pallas_call(
        functools.partial(gate_kernel, n, cores),
        in_specs=[SMEM_SPEC] + [VMEM_SPEC] * (len(blocks) + 2),
        out_specs=VMEM_SPEC,
        out_shape=jax.ShapeDtypeStruct((width, cores * rows), jnp.bfloat16),
        compiler_params=pltpu.CompilerParams(vmem_limit_bytes=10 << 20),
        cost_estimate=pl.CostEstimate(
            flops=4 * rows * cores * D * width * 2,
            transcendentals=rows * cores * width,
            bytes_accessed=4 * D * width,
        ),
    )(place, *blocks, w_gate, w_up)


def run_down(blocks, active, n, cores, place, w_down, experts):
    rows = blocks[0].shape[0]
    width = w_down.shape[1]
    shape = jax.ShapeDtypeStruct((n, rows, width), jnp.bfloat16)
    return pl.pallas_call(
        functools.partial(down_kernel, n, cores, experts),
        in_specs=[SMEM_SPEC] + [VMEM_SPEC] * (len(blocks) + 2),
        out_specs=(VMEM_SPEC,) * cores,
        out_shape=(shape,) * cores,
        compiler_params=pltpu.CompilerParams(vmem_limit_bytes=10 << 20),
        cost_estimate=pl.CostEstimate(
            flops=2 * rows * cores * D * width * 2,
            transcendentals=0,
            bytes_accessed=2 * D * width,
        ),
    )(place, *blocks, active, w_down)


def held(x):
    return pltpu.with_memory_space_constraint(x, pltpu.VMEM)


def shards(
    queries,
    row_key_value,
    shared_context_cache,
    branch,
    sink_logits,
    w_out,
    residual,
    norm_gain,
    expert_ids,
    weight_codes,
    w_gate,
    w_up,
    w_down,
):
    n = lax.axis_size("att")
    senders = lax.axis_size("exp")
    experts = w_gate.shape[0] * senders
    assert w_gate.shape[0] == 1 and n & (n - 1) == 0 and senders & (senders - 1) == 0
    cores = 2
    chips = senders // cores
    part = lax.axis_index("att")
    place = jnp.stack([part, lax.axis_index("exp")]).astype(jnp.int32)

    def over_att(x, k):
        return lax.ppermute(x, "att", [(i, i ^ k) for i in range(n)])

    def over_exp(x, k):
        return lax.ppermute(x, "exp", [(i, i ^ k) for i in range(senders)])

    w_out = pltpu.with_memory_space_constraint(w_out.T, pltpu.HBM)
    queries = pltpu.with_memory_space_constraint(queries, pltpu.HBM)
    cache = pltpu.with_memory_space_constraint(shared_context_cache, pltpu.HBM)
    own = pltpu.with_memory_space_constraint(row_key_value, pltpu.HBM)
    w_gate = held(jnp.swapaxes(w_gate, 1, 2))
    w_up = held(jnp.swapaxes(w_up, 1, 2))
    w_down = held(w_down)
    w_parts = []
    gathered = []
    for chunk in range(CHUNKS):
        mine, w_part = attend(chunk, place, sink_logits, branch[None, :], queries, cache, own, w_out)
        w_parts.append(w_part)
        gathered.append([mine] + [over_att(mine, k) for k in range(1, n)])
    so_far = project(gathered[0], w_parts[0])
    attended, packed = finish(
        gathered[1],
        w_parts[1],
        so_far,
        residual,
        norm_gain[None, :],
        expert_ids.T,
        weight_codes.T,
        experts,
    )
    far = {c: over_exp(packed, c * cores) for c in range(chips - 1, 0, -1)}
    near = [packed] + [far[c] for c in range(1, chips)]
    sides, twins = {}, {}
    for c in range(chips):
        sides[c] = [near[c]] + [over_att(near[c], k) for k in range(1, n)]
        twins[c] = [over_exp(b, 1) for b in sides[c]]
    batches = [[c] for c in range(chips - 1, 2, -1)] + [[2, 1] if chips > 2 else [1], [0]]
    homes = []
    for batch in batches:
        blocks = sum([sides[c] for c in batch], []) + sum([twins[c] for c in batch], [])
        groups = len(batch) * cores
        active = run_gate(blocks, n, groups, place, w_gate, w_up)
        outs = run_down(blocks[::n], active, n, groups, place, w_down, experts)
        place = lax.optimization_barrier((place, outs[0]))[0]
        for i, c in enumerate(batch):
            other = over_exp(outs[len(batch) + i], 1)
            summed = outs[i].astype(jnp.float32) + other.astype(jnp.float32)
            mine = summed[0]
            for k in range(1, n):
                mine = mine + over_att(summed[k].astype(jnp.bfloat16), k).astype(jnp.float32)
            if c > 0:
                mine = over_exp(mine.astype(jnp.bfloat16), c * cores)
            homes.append(mine.astype(jnp.float32))
    home = functools.reduce(jnp.add, homes)
    return (attended, home.astype(jnp.bfloat16))


def solution(mesh):
    placed = (
        P(("groups", "exp"), None),
        P(("groups", "exp"), None),
        P("groups", "att", None),
        P(("groups", "exp")),
        P(),
        P(None, "att"),
        P(("groups", "exp"), "att"),
        P("att"),
        P(("groups", "exp"), None),
        P(("groups", "exp"), None),
        P("exp", None, "att"),
        P("exp", None, "att"),
        P("exp", "att", None),
    )
    return jax.shard_map(
        shards,
        mesh=mesh,
        in_specs=placed,
        out_specs=(P(("groups", "exp"), "att"), P(("groups", "exp"), "att")),
        check_vma=False,
    )
```
